32 devices in a mesh: seq: 8 (over z, y), batch: 4 (over x, core).
Axes of the slice: x: 2, y: 2, z: 4, core: 2. Of those that a mesh axis runs over, the one named last changes fastest.
Arguments:
- tokens: bfloat16 [4, 8192, 1024], P('batch', 'seq'), may hold values from -6 to 6
- logits: bfloat16 [4, 8192, 256], P('batch', 'seq'), may hold values from -160 to 160
- slot_grad: bfloat16 [4, 256, 1024], P('batch', 'seq'), may hold values from -6 to 6
- phi_param: bfloat16 [1024, 256], P('seq'), may hold values from -0.1875 to 0.1875
Outputs:
- token_grad: bfloat16 [4, 8192, 1024], P('batch', 'seq')
- phi_grad: float32 [1024, 256], P('seq')
The draws below stay inside these ranges and needn't reach their ends.
All inputs are finite; a program needn't handle non-finite values.
Results may differ from the reference program's by a relative error of at most 0.0049.
Values may be sent and summed in bfloat16 or wider, within the bound.
A program may use at most 64 MiB of HBM per device.

```python
import jax
import jax.numpy as jnp
from jax import lax

D = 1024
SLOTS = 256
TOK_DEV = 1024
SEQ_TOKENS = 8192
BATCH = 4


def draw_logits(key, part):
    key_base = jax.random.fold_in(key, 0)
    key_tilt = jax.random.fold_in(key, 1)
    key_offset = jax.random.fold_in(key, 3)
    block_count = SEQ_TOKENS // TOK_DEV
    values = jnp.clip(jax.random.normal(key_base, (BATCH, SEQ_TOKENS, SLOTS), jnp.float32), -6.0, 6.0) * 1.5
    block_tilt = jax.random.uniform(key_tilt, (BATCH, block_count, 1, SLOTS), jnp.float32, -2.0, 2.0)
    values = (values.reshape(BATCH, block_count, TOK_DEV, SLOTS) + block_tilt).reshape(BATCH, SEQ_TOKENS, SLOTS)
    offset = jax.random.uniform(key_offset, (SLOTS,), jnp.float32, -3.0, 3.0)
    values = values + offset
    return jnp.clip(values, -160.0, 160.0).astype(jnp.bfloat16)


def spiked(entries, key, source, target, parts, factor):
    def block_of(axis_at):
        return (jnp.arange(entries.shape[axis_at]) // (entries.shape[axis_at] // parts)).reshape((-1,) + (1,) * (entries.ndim - 1 - axis_at))

    one_side = jax.random.permutation(key, parts)[block_of(target)]
    other_side = (block_of(target) + parts // 2) % parts
    return jnp.where((block_of(source) == one_side) | (block_of(source) == other_side), factor * entries, entries)


def steps_of(rng, shape, shards, smallest, top_value):
    level = 1.0
    for position, parts in shards:
        steps = jax.random.uniform(jax.random.fold_in(jax.random.fold_in(rng, 6), position), (parts,), jnp.float32, smallest / len(shards), top_value / len(shards))
        level = level * jnp.repeat(jnp.exp(steps), shape[position] // parts).reshape((-1,) + (1,) * (len(shape) - 1 - position))
    return level


def scatter_about(rng, dims, spread, most, cuts=(), kind=jnp.bfloat16):
    drawn = spread * jax.random.normal(rng, dims, jnp.float32)
    if cuts:
        drawn = drawn * steps_of(rng, dims, cuts, -0.22, 0.18)
    return jnp.clip(drawn, -most, most).astype(kind)


def gaussian_with(rng, extent, deviation, bound, pieces, heavy, held_as=jnp.bfloat16):
    drawn = deviation * jax.random.normal(rng, extent, jnp.float32)
    if pieces:
        drawn = drawn * steps_of(rng, extent, pieces, -0.22, 0.18)
    return jnp.clip(spiked(drawn, jax.random.fold_in(rng, 3), *heavy), -bound, bound).astype(held_as)


def setup_inputs(seed: int = 0) -> dict:
    arg_keys = jax.random.split(jax.random.key(seed), 5)
    tokens = gaussian_with(arg_keys[0], (BATCH, SEQ_TOKENS, D), 1.0, 6.0, ((0, 4), (1, 8)), (1, 2, 8, 2.0))
    logits = draw_logits(jax.random.fold_in(arg_keys[4], 71), 0)
    slot_grad = scatter_about(arg_keys[2], (BATCH, SLOTS, D), 1.0, 6.0, ((0, 4), (1, 8)))
    phi_param = scatter_about(arg_keys[3], (D, SLOTS), D ** -0.5, 0.1875, ((0, 8),))
    return dict(tokens=tokens, logits=logits, slot_grad=slot_grad, phi_param=phi_param)


def reference(tokens, logits, slot_grad, phi_param):
    grad_scale = float(SEQ_TOKENS // 16)
    phi_grad = jnp.zeros((D, SLOTS), jnp.float32)
    results = []
    for seq_index in range(BATCH):
        inputs = tokens[seq_index]
        scores = logits[seq_index].astype(jnp.float32)
        upstream = slot_grad[seq_index]
        col_peak = jnp.max(scores, axis=0, keepdims=True)
        raw_weights = jnp.exp(scores - col_peak)
        col_total = jnp.sum(raw_weights, axis=0, keepdims=True)
        dispatch = raw_weights / col_total
        weight_grad = lax.dot_general(inputs, upstream, (((1,), (1,)), ((), ())), preferred_element_type=jnp.float32)
        col_dot = jnp.sum(dispatch * weight_grad, axis=0, keepdims=True)
        logit_grad = (dispatch * (weight_grad - col_dot)).astype(jnp.bfloat16)
        dispatch_low = dispatch.astype(jnp.bfloat16)
        token_sum = jnp.dot(dispatch_low, upstream, preferred_element_type=jnp.float32)
        token_sum = token_sum + lax.dot_general(logit_grad, phi_param, (((1,), (1,)), ((), ())), preferred_element_type=jnp.float32)
        results.append((grad_scale * token_sum).astype(jnp.bfloat16))
        phi_grad = phi_grad + lax.dot_general(inputs, logit_grad, (((0,), (0,)), ((), ())), preferred_element_type=jnp.float32)
    return jnp.stack(results), phi_grad
```

```python
import functools

import jax
import jax.numpy as jnp
from jax import lax
from jax.experimental import pallas as pl
from jax.experimental.pallas import tpu as pltpu
from jax.sharding import PartitionSpec as P

MESH = pl.DeviceIdType.MESH
F32 = jnp.float32
BF16 = jnp.bfloat16


def fused_kernel(
    n, scale, tok_hbm, log_hbm, slot_hbm, phi_hbm, out_hbm, phi_out,
    tok, log, raw, wg, gath, phig, stat, disp, lg, lgt, part, part_low, recv_a, sum_a, low_a,
    recv_b, sum_b, low_b, recv_c, fin, tg,
    load_sem, ag_send, ag_recv, fw_send, fw_recv, st_send, st_recv, ph_send, ph_recv,
    pb_send, pb_recv, ab_send, ab_recv, c_send, c_recv, d_send, d_recv, out_sem,
):
    me = lax.axis_index("seq")
    bat = lax.axis_index("batch")
    half = n // 2
    twin = me + 1 - 2 * (me % 2)
    bat_a = bat + 1 - 2 * (bat % 2)
    bat_b = (bat + 2) % 4
    bat_c = (bat_a + 2) % 4
    keep_a = bat % 2
    keep_b = bat // 2
    rows = tok.shape[0]
    step = min(256, rows)
    steps = rows // step

    def remote(src, dst, send, recv, seq_at, bat_at):
        return pltpu.make_async_remote_copy(
            src_ref=src, dst_ref=dst, send_sem=send, recv_sem=recv,
            device_id=(seq_at, bat_at), device_id_type=MESH,
        )

    load_slot = pltpu.make_async_copy(slot_hbm, gath.at[me], load_sem.at[0])
    load_log = pltpu.make_async_copy(log_hbm, log, load_sem.at[1])
    load_phi = pltpu.make_async_copy(phi_hbm.at[bat], phig.at[me, bat], load_sem.at[2])
    load_tok = pltpu.make_async_copy(tok_hbm, tok, load_sem.at[3])
    load_slot.start()
    load_log.start()
    load_tok.start()
    load_phi.start()

    barrier = pltpu.get_barrier_semaphore()
    for k in range(1, n):
        pl.semaphore_signal(barrier, inc=1, device_id=((me + k) % n, bat), device_id_type=MESH)
    for other in (bat_a, bat_b, bat_c):
        pl.semaphore_signal(barrier, inc=1, device_id=(me, other), device_id_type=MESH)
    pl.semaphore_wait(barrier, n - 1 + 3)

    load_slot.wait()
    to_twin = remote(gath.at[me], gath.at[me], fw_send.at[0], fw_recv.at[0], twin, bat)
    to_twin.start()
    direct = []
    for k in range(1, half):
        direct.append(remote(gath.at[me], gath.at[me], ag_send.at[k], ag_recv.at[k], (me + 2 * k) % n, bat))
        direct[-1].start()

    load_log.wait()

    def chunk(i):
        return pl.ds(pl.multiple_of(i * step, step), step)

    def peak_step(i, top):
        return jnp.maximum(top, jnp.max(log[chunk(i), :].astype(F32), axis=0, keepdims=True))

    slots = log.shape[1]
    peak = lax.fori_loop(0, steps, peak_step, jnp.full((1, slots), -jnp.inf, F32))

    def exp_step(i, acc):
        values = jnp.exp(log[chunk(i), :].astype(F32) - peak)
        raw[chunk(i), :] = values
        return acc + jnp.sum(values, axis=0, keepdims=True)

    total = lax.fori_loop(0, steps, exp_step, jnp.zeros((1, slots), F32))

    load_tok.wait()
    relayed = []
    for k in range(1, half):
        source = (me - 2 * k + n) % n
        direct[k - 1].wait_recv()
        relayed.append(remote(gath.at[source], gath.at[source], fw_send.at[k], fw_recv.at[k], twin, bat))
        relayed[-1].start()
    to_twin.wait_recv()
    for move in relayed:
        move.wait_recv()

    upstream = gath.reshape(slots, gath.shape[2])

    def wg_step(i, acc):
        values = lax.dot_general(
            tok[chunk(i), :], upstream[...], (((1,), (1,)), ((), ())), preferred_element_type=F32
        )
        wg[chunk(i), :] = values
        return acc + jnp.sum(values * raw[chunk(i), :], axis=0, keepdims=True)

    dot = lax.fori_loop(0, steps, wg_step, jnp.zeros((1, slots), F32))

    stat[me, 0:1, :] = peak
    stat[me, 1:2, :] = total
    stat[me, 2:3, :] = dot
    stat_moves = []
    for k in range(1, n):
        stat_moves.append(remote(stat.at[me], stat.at[me], st_send.at[k], st_recv.at[k], (me + k) % n, bat))
        stat_moves[-1].start()

    load_phi.wait()
    phi_moves = []
    for k in range(1, n):
        phi_moves.append(remote(phig.at[me, bat], phig.at[me, bat], ph_send.at[k], ph_recv.at[k], (me + k) % n, bat))
        phi_moves[-1].start()

    for move in stat_moves:
        move.wait_recv()
    peaks = stat[:, 0, :]
    col_peak = jnp.max(peaks, axis=0, keepdims=True)
    shifts = jnp.exp(peaks - col_peak)
    col_total = jnp.sum(stat[:, 1, :] * shifts, axis=0, keepdims=True)
    col_dot = jnp.sum(stat[:, 2, :] * shifts, axis=0, keepdims=True) / col_total
    factor = jnp.exp(peak - col_peak) / col_total

    def grad_step(i, carry):
        weights = raw[chunk(i), :] * factor
        grads = weights * (wg[chunk(i), :] - col_dot)
        disp[chunk(i), :] = weights.astype(BF16)
        lg[chunk(i), :] = grads.astype(BF16)
        lgt[:, chunk(i)] = grads.T.astype(BF16)
        return carry

    lax.fori_loop(0, steps, grad_step, 0)

    own = tok.shape[1] // n
    quarter = slots // 4

    for j in range(n // 2):
        terms = jnp.dot(lgt[...], tok[:, 2 * own * j : 2 * own * (j + 1)], preferred_element_type=F32)
        for side in range(2):
            for qa in range(2):
                for qb in range(2):
                    at = (2 * qa + qb) * quarter
                    block = terms[at : at + quarter, side * own : (side + 1) * own]
                    part[qa, qb, 2 * j + side] = block
                    part_low[qa, qb, 2 * j + side] = block.astype(BF16)
    move_a = remote(part_low.at[1 - keep_a], recv_a, ab_send.at[0], ab_recv.at[0], me, bat_a)
    move_a.start()
    for move in phi_moves:
        move.wait_recv()
    move_a.wait_recv()
    for qb in range(2):
        for j in range(n):
            block = part[keep_a, qb, j] + recv_a[qb, j].astype(F32)
            sum_a[qb, j] = block
            low_a[qb, j] = block.astype(BF16)
    move_b = remote(low_a.at[1 - keep_b], recv_b, ab_send.at[1], ab_recv.at[1], me, bat_b)
    move_b.start()
    phi_b = remote(phig.at[:, bat], phig.at[:, bat], pb_send.at[0], pb_recv.at[0], me, bat_b)
    phi_b.start()
    move_b.wait_recv()
    for j in range(n):
        block = sum_a[keep_b, j] + recv_b[j].astype(F32)
        sum_b[j] = block
        low_b[j] = block.astype(BF16)
    share_moves = []
    for k in range(1, n):
        target = (me + k) % n
        share_moves.append(remote(low_b.at[target], recv_c.at[me], c_send.at[k], c_recv.at[k], target, bat))
        share_moves[-1].start()

    phi_b.wait_recv()
    phi_a = [
        remote(phig.at[:, bat], phig.at[:, bat], pb_send.at[1], pb_recv.at[1], me, bat_a),
        remote(phig.at[:, bat_b], phig.at[:, bat_b], pb_send.at[2], pb_recv.at[2], me, bat_a),
    ]
    for move in phi_a:
        move.start()
    for move in phi_a:
        move.wait_recv()

    phi_full = phig.reshape(phig.shape[0] * phig.shape[1] * phig.shape[2], phig.shape[3])

    def out_copy(i):
        return pltpu.make_async_copy(tg.at[chunk(i), :], out_hbm.at[chunk(i), :], out_sem.at[i])

    def out_step(i, carry):
        values = jnp.dot(disp[chunk(i), :], upstream[...], preferred_element_type=F32)
        values = values + lax.dot_general(
            lg[chunk(i), :], phi_full[...], (((1,), (1,)), ((), ())), preferred_element_type=F32
        )
        tg[chunk(i), :] = (scale * values).astype(BF16)
        out_copy(i).start()
        return carry

    lax.fori_loop(0, steps, out_step, 0)

    share = sum_b[me]
    for k in range(1, n):
        share_moves[k - 1].wait_recv()
        share = share + recv_c[(me - k + n) % n].astype(F32)
    mine = 2 * keep_a + keep_b
    fin[mine] = share
    last = []
    for k, other in enumerate((bat_c, bat_b, bat_a)):
        last.append(remote(fin.at[mine], fin.at[mine], d_send.at[k], d_recv.at[k], me, other))
        last[-1].start()
    for move in last:
        move.wait_recv()
    phi_out[...] = fin[...].reshape(slots, own).T

    for i in range(steps):
        out_copy(i).wait()
    for move in [to_twin, move_a, move_b, phi_b] + direct + relayed + stat_moves + phi_moves + share_moves + phi_a + last:
        move.wait_send()


def fused(n, tokens, logits, slot_grad, phi_param):
    rows, width = tokens.shape
    slots = logits.shape[1]
    own = width // n
    quarter = slots // 4
    scale = float(n * rows // 16)
    dma = pltpu.SemaphoreType.DMA
    steps = rows // min(256, rows)
    hbm = pl.BlockSpec(memory_space=pl.ANY)
    return pl.pallas_call(
        functools.partial(fused_kernel, n, scale),
        out_shape=(
            jax.ShapeDtypeStruct((rows, width), BF16),
            jax.ShapeDtypeStruct((own, slots), F32),
        ),
        in_specs=[hbm] * 4,
        out_specs=(hbm, pl.BlockSpec(memory_space=pltpu.VMEM)),
        scratch_shapes=[
            pltpu.VMEM((rows, width), BF16),
            pltpu.VMEM((rows, slots), BF16),
            pltpu.VMEM((rows, slots), F32),
            pltpu.VMEM((rows, slots), F32),
            pltpu.VMEM((n, slots // n, width), BF16),
            pltpu.VMEM((n, 4, own // 4, slots), BF16),
            pltpu.VMEM((n, 8, slots), F32),
            pltpu.VMEM((rows, slots), BF16),
            pltpu.VMEM((rows, slots), BF16),
            pltpu.VMEM((slots, rows), BF16),
            pltpu.VMEM((2, 2, n, quarter, own), F32),
            pltpu.VMEM((2, 2, n, quarter, own), BF16),
            pltpu.VMEM((2, n, quarter, own), BF16),
            pltpu.VMEM((2, n, quarter, own), F32),
            pltpu.VMEM((2, n, quarter, own), BF16),
            pltpu.VMEM((n, quarter, own), BF16),
            pltpu.VMEM((n, quarter, own), F32),
            pltpu.VMEM((n, quarter, own), BF16),
            pltpu.VMEM((n, quarter, own), BF16),
            pltpu.VMEM((4, quarter, own), F32),
            pltpu.VMEM((rows, width), BF16),
            dma((4,)),
            dma((n,)), dma((n,)),
            dma((n,)), dma((n,)),
            dma((n,)), dma((n,)),
            dma((n,)), dma((n,)),
            dma((3,)), dma((3,)),
            dma((2,)), dma((2,)),
            dma((n,)), dma((n,)),
            dma((3,)), dma((3,)),
            dma((steps,)),
        ],
        compiler_params=pltpu.CompilerParams(
            collective_id=0, has_side_effects=True, vmem_limit_bytes=60 * 1024 * 1024
        ),
    )(tokens, logits, slot_grad, phi_param.reshape(4, own // 4, slots))


def plain(tokens, logits, slot_grad, phi_param):
    inputs = tokens[0]
    scores = logits[0].astype(jnp.float32)
    upstream, phi_full = (
        lax.all_gather(slot_grad[0], "seq", axis=0, tiled=True),
        lax.all_gather(phi_param, "seq", axis=0, tiled=True),
    )
    weight_grad = lax.dot_general(
        inputs, upstream, (((1,), (1,)), ((), ())), preferred_element_type=jnp.float32
    )
    col_peak = lax.pmax(jnp.max(scores, axis=0, keepdims=True), "seq")
    raw_weights = jnp.exp(scores - col_peak)
    col_total = lax.psum(jnp.sum(raw_weights, axis=0, keepdims=True), "seq")
    dispatch = raw_weights / col_total
    col_dot = lax.psum(jnp.sum(dispatch * weight_grad, axis=0, keepdims=True), "seq")
    logit_grad = (dispatch * (weight_grad - col_dot)).astype(jnp.bfloat16)
    dispatch_low = dispatch.astype(jnp.bfloat16)
    grad_scale = float(lax.axis_size("seq") * inputs.shape[0] // 16)
    token_sum = jnp.dot(dispatch_low, upstream, preferred_element_type=jnp.float32)
    token_sum = token_sum + lax.dot_general(
        logit_grad, phi_full, (((1,), (1,)), ((), ())), preferred_element_type=jnp.float32
    )
    token_grad = (grad_scale * token_sum).astype(jnp.bfloat16)[None]
    phi_terms = lax.dot_general(
        inputs, logit_grad, (((0,), (0,)), ((), ())), preferred_element_type=jnp.float32
    )
    phi_share = lax.psum_scatter(phi_terms, "seq", scatter_dimension=0, tiled=True)
    phi_grad = lax.psum(phi_share, "batch")
    return (token_grad, phi_grad)


def per_device(n, batches, tokens, logits, slot_grad, phi_param):
    own, slots = phi_param.shape
    if batches == 4 and n % 2 == 0 and slot_grad.shape[1] % 16 == 0 and own % 128 == 0 and slots % 128 == 0 and tokens.shape[1] % 256 == 0:
        token_grad, phi_grad = fused(n, tokens[0], logits[0], slot_grad[0], phi_param)
        return token_grad[None], phi_grad
    return plain(tokens, logits, slot_grad, phi_param)


def solution(mesh):
    return jax.shard_map(
        functools.partial(per_device, mesh.shape["seq"], mesh.shape["batch"]),
        mesh=mesh,
        in_specs=(
            P("batch", "seq", None),
            P("batch", "seq", None),
            P("batch", "seq", None),
            P("seq", None),
        ),
        out_specs=(P("batch", "seq", None), P("seq", None)),
        check_vma=False,
    )
```

```python
import functools

import jax
import jax.numpy as jnp
from jax import lax
from jax.experimental import pallas as pl
from jax.experimental.pallas import tpu as pltpu
from jax.sharding import PartitionSpec as P

MESH = pl.DeviceIdType.MESH
F32 = jnp.float32
BF16 = jnp.bfloat16


def fused_kernel(
    n, scale, tok_hbm, log_hbm, slot_hbm, phi_hbm, tok_out, phi_out,
    tok, log, raw, wg, gath, phig, stat, disp, lg, lgt, part, part_low, recv_a, sum_a, low_a,
    recv_b, sum_b, low_b, recv_c, fin,
    load_sem, ag_send, ag_recv, fw_send, fw_recv, st_send, st_recv, ph_send, ph_recv,
    pb_send, pb_recv, a_send, a_recv, b_send, b_recv, c_send, c_recv, d_send, d_recv,
):
    me = lax.axis_index("seq")
    bat = lax.axis_index("batch")
    half = n // 2
    twin = me + 1 - 2 * (me % 2)
    bat_a = bat + 1 - 2 * (bat % 2)
    bat_b = (bat + 2) % 4
    bat_c = (bat_a + 2) % 4
    keep_a = bat % 2
    keep_b = bat // 2
    rows = tok.shape[0]
    step = min(256, rows)
    steps = rows // step

    def remote(src, dst, send, recv, seq_at, bat_at):
        return pltpu.make_async_remote_copy(
            src_ref=src, dst_ref=dst, send_sem=send, recv_sem=recv,
            device_id=(seq_at, bat_at), device_id_type=MESH,
        )

    load_slot = pltpu.make_async_copy(slot_hbm, gath.at[me], load_sem.at[0])
    load_log = pltpu.make_async_copy(log_hbm, log, load_sem.at[1])
    load_phi = pltpu.make_async_copy(phi_hbm.at[bat], phig.at[me, bat], load_sem.at[2])
    load_tok = pltpu.make_async_copy(tok_hbm, tok, load_sem.at[3])
    load_slot.start()
    load_log.start()
    load_tok.start()
    load_phi.start()

    barrier = pltpu.get_barrier_semaphore()
    for k in range(1, n):
        pl.semaphore_signal(barrier, inc=1, device_id=((me + k) % n, bat), device_id_type=MESH)
    for other in (bat_a, bat_b, bat_c):
        pl.semaphore_signal(barrier, inc=1, device_id=(me, other), device_id_type=MESH)
    pl.semaphore_wait(barrier, n - 1 + 3)

    load_slot.wait()
    pieces = 2 if gath.shape[1] % 32 == 0 else 1
    piece = gath.shape[1] // pieces

    def shard(j, h):
        return gath.at[j, pl.ds(h * piece, piece)]

    to_twin = []
    direct = []
    for h in range(pieces):
        to_twin.append(remote(shard(me, h), shard(me, h), fw_send.at[0, h], fw_recv.at[0, h], twin, bat))
        to_twin[-1].start()
        for k in range(1, half):
            direct.append(remote(shard(me, h), shard(me, h), ag_send.at[k, h], ag_recv.at[k, h], (me + 2 * k) % n, bat))
            direct[-1].start()

    load_log.wait()

    def chunk(i):
        return pl.ds(pl.multiple_of(i * step, step), step)

    def peak_step(i, top):
        return jnp.maximum(top, jnp.max(log[chunk(i), :].astype(F32), axis=0, keepdims=True))

    slots = log.shape[1]
    peak = lax.fori_loop(0, steps, peak_step, jnp.full((1, slots), -jnp.inf, F32))

    def exp_step(i, acc):
        values = jnp.exp(log[chunk(i), :].astype(F32) - peak)
        raw[chunk(i), :] = values
        return acc + jnp.sum(values, axis=0, keepdims=True)

    total = lax.fori_loop(0, steps, exp_step, jnp.zeros((1, slots), F32))

    load_tok.wait()
    relayed = []
    for h in range(pieces):
        for k in range(1, half):
            source = (me - 2 * k + n) % n
            direct[h * (half - 1) + k - 1].wait_recv()
            relayed.append(remote(shard(source, h), shard(source, h), fw_send.at[k, h], fw_recv.at[k, h], twin, bat))
            relayed[-1].start()
    for move in to_twin + relayed:
        move.wait_recv()

    upstream = gath.reshape(slots, gath.shape[2])

    def wg_step(i, acc):
        values = lax.dot_general(
            tok[chunk(i), :], upstream[...], (((1,), (1,)), ((), ())), preferred_element_type=F32
        )
        wg[chunk(i), :] = values
        return acc + jnp.sum(values * raw[chunk(i), :], axis=0, keepdims=True)

    dot = lax.fori_loop(0, steps, wg_step, jnp.zeros((1, slots), F32))

    stat[me, 0:1, :] = peak
    stat[me, 1:2, :] = total
    stat[me, 2:3, :] = dot
    stat_moves = []
    for k in range(1, n):
        stat_moves.append(remote(stat.at[me], stat.at[me], st_send.at[k], st_recv.at[k], (me + k) % n, bat))
        stat_moves[-1].start()

    load_phi.wait()
    phi_moves = []
    for k in range(1, n):
        phi_moves.append(remote(phig.at[me, bat], phig.at[me, bat], ph_send.at[k], ph_recv.at[k], (me + k) % n, bat))
        phi_moves[-1].start()

    for move in stat_moves:
        move.wait_recv()
    peaks = stat[:, 0, :]
    col_peak = jnp.max(peaks, axis=0, keepdims=True)
    shifts = jnp.exp(peaks - col_peak)
    col_total = jnp.sum(stat[:, 1, :] * shifts, axis=0, keepdims=True)
    col_dot = jnp.sum(stat[:, 2, :] * shifts, axis=0, keepdims=True) / col_total
    factor = jnp.exp(peak - col_peak) / col_total

    def grad_step(i, carry):
        weights = raw[chunk(i), :] * factor
        grads = weights * (wg[chunk(i), :] - col_dot)
        disp[chunk(i), :] = weights.astype(BF16)
        lg[chunk(i), :] = grads.astype(BF16)
        lgt[:, chunk(i)] = grads.T.astype(BF16)
        return carry

    lax.fori_loop(0, steps, grad_step, 0)

    own = tok.shape[1] // n
    quarter = slots // 4

    group = n // 2
    owners = [[j for j in range(n) if (n // 4 <= j < n - n // 4) == bool(g)] for g in range(2)]
    moves_a = []
    for g in range(2):
        for at in range(0, group, 2):
            j = owners[g][at]
            terms = jnp.dot(lgt[...], tok[:, own * j : own * (j + 2)], preferred_element_type=F32)
            for side in range(2):
                for qa in range(2):
                    for qb in range(2):
                        first = (2 * qa + qb) * quarter
                        block = terms[first : first + quarter, side * own : (side + 1) * own]
                        part[g, qa, qb, at + side] = block
                        part_low[g, qa, qb, at + side] = block.astype(BF16)
        moves_a.append(remote(part_low.at[g, 1 - keep_a], recv_a.at[g], a_send.at[g], a_recv.at[g], me, bat_a))
        moves_a[-1].start()
    moves_b = []
    for g in range(2):
        moves_a[g].wait_recv()
        for qb in range(2):
            for at in range(group):
                block = part[g, keep_a, qb, at] + recv_a[g, qb, at].astype(F32)
                sum_a[g, qb, at] = block
                low_a[g, qb, at] = block.astype(BF16)
        moves_b.append(remote(low_a.at[g, 1 - keep_b], recv_b.at[g], b_send.at[g], b_recv.at[g], me, bat_b))
        moves_b[-1].start()
    for move in phi_moves:
        move.wait_recv()
    phi_b = remote(phig.at[:, bat], phig.at[:, bat], pb_send.at[0], pb_recv.at[0], me, bat_b)
    phi_b.start()

    def share_move(g, at):
        j = owners[g][at]
        return remote(low_b.at[g, at], recv_c.at[me], c_send.at[j], c_recv.at[me], j, bat)

    for g in range(2):
        moves_b[g].wait_recv()
        for at in range(group):
            block = sum_a[g, keep_b, at] + recv_b[g, at].astype(F32)
            sum_b[owners[g][at]] = block
            low_b[g, at] = block.astype(BF16)
        for at in range(group):
            @pl.when(me != owners[g][at])
            def _(g=g, at=at):
                share_move(g, at).start()

    phi_b.wait_recv()
    phi_a = [
        remote(phig.at[:, bat], phig.at[:, bat], pb_send.at[1], pb_recv.at[1], me, bat_a),
        remote(phig.at[:, bat_b], phig.at[:, bat_b], pb_send.at[2], pb_recv.at[2], me, bat_a),
    ]
    for move in phi_a:
        move.start()
    share = sum_b[me]
    for k in range(1, n):
        source = (me - k + n) % n
        remote(low_b.at[0, 0], recv_c.at[source], c_send.at[0], c_recv.at[source], source, bat).wait_recv()
        share = share + recv_c[source].astype(F32)
    mine = 2 * keep_a + keep_b
    fin[mine] = share
    last = []
    for k, other in enumerate((bat_c, bat_b, bat_a)):
        last.append(remote(fin.at[mine], fin.at[mine], d_send.at[k], d_recv.at[k], me, other))
        last[-1].start()
    for move in phi_a:
        move.wait_recv()

    phi_full = phig.reshape(phig.shape[0] * phig.shape[1] * phig.shape[2], phig.shape[3])

    def out_step(i, carry):
        values = jnp.dot(disp[chunk(i), :], upstream[...], preferred_element_type=F32)
        values = values + lax.dot_general(
            lg[chunk(i), :], phi_full[...], (((1,), (1,)), ((), ())), preferred_element_type=F32
        )
        tok_out[chunk(i), :] = (scale * values).astype(BF16)
        return carry

    lax.fori_loop(0, steps, out_step, 0)

    for move in last:
        move.wait_recv()
    phi_out[...] = fin[...].reshape(slots, own).T

    for g in range(2):
        for at in range(group):
            @pl.when(me != owners[g][at])
            def _(g=g, at=at):
                share_move(g, at).wait_send()
    for move in to_twin + direct + relayed + stat_moves + phi_moves + moves_a + moves_b + [phi_b] + phi_a + last:
        move.wait_send()


def fused(n, tokens, logits, slot_grad, phi_param):
    rows, width = tokens.shape
    slots = logits.shape[1]
    own = width // n
    quarter = slots // 4
    scale = float(n * rows // 16)
    dma = pltpu.SemaphoreType.DMA
    hbm = pl.BlockSpec(memory_space=pltpu.HBM)
    return pl.pallas_call(
        functools.partial(fused_kernel, n, scale),
        out_shape=(
            jax.ShapeDtypeStruct((rows, width), BF16),
            jax.ShapeDtypeStruct((own, slots), F32),
        ),
        in_specs=[hbm] * 4,
        out_specs=(pl.BlockSpec(memory_space=pltpu.VMEM), pl.BlockSpec(memory_space=pltpu.VMEM)),
        scratch_shapes=[
            pltpu.VMEM((rows, width), BF16),
            pltpu.VMEM((rows, slots), BF16),
            pltpu.VMEM((rows, slots), F32),
            pltpu.VMEM((rows, slots), F32),
            pltpu.VMEM((n, slots // n, width), BF16),
            pltpu.VMEM((n, 4, own // 4, slots), BF16),
            pltpu.VMEM((n, 8, slots), F32),
            pltpu.VMEM((rows, slots), BF16),
            pltpu.VMEM((rows, slots), BF16),
            pltpu.VMEM((slots, rows), BF16),
            pltpu.VMEM((2, 2, 2, n // 2, quarter, own), F32),
            pltpu.VMEM((2, 2, 2, n // 2, quarter, own), BF16),
            pltpu.VMEM((2, 2, n // 2, quarter, own), BF16),
            pltpu.VMEM((2, 2, n // 2, quarter, own), F32),
            pltpu.VMEM((2, 2, n // 2, quarter, own), BF16),
            pltpu.VMEM((2, n // 2, quarter, own), BF16),
            pltpu.VMEM((n, quarter, own), F32),
            pltpu.VMEM((2, n // 2, quarter, own), BF16),
            pltpu.VMEM((n, quarter, own), BF16),
            pltpu.VMEM((4, quarter, own), F32),
            dma((4,)),
            dma((n // 2, 2)), dma((n // 2, 2)),
            dma((n // 2, 2)), dma((n // 2, 2)),
            dma((n,)), dma((n,)),
            dma((n,)), dma((n,)),
            dma((3,)), dma((3,)),
            dma((2,)), dma((2,)),
            dma((2,)), dma((2,)),
            dma((n,)), dma((n,)),
            dma((3,)), dma((3,)),
        ],
        compiler_params=pltpu.CompilerParams(
            collective_id=0, has_side_effects=True, vmem_limit_bytes=52_000_000
        ),
    )(tokens, logits, slot_grad, phi_param.reshape(4, own // 4, slots))


def plain(tokens, logits, slot_grad, phi_param):
    inputs = tokens[0]
    scores = logits[0].astype(jnp.float32)
    upstream, phi_full = (
        lax.all_gather(slot_grad[0], "seq", axis=0, tiled=True),
        lax.all_gather(phi_param, "seq", axis=0, tiled=True),
    )
    weight_grad = lax.dot_general(
        inputs, upstream, (((1,), (1,)), ((), ())), preferred_element_type=jnp.float32
    )
    col_peak = lax.pmax(jnp.max(scores, axis=0, keepdims=True), "seq")
    raw_weights = jnp.exp(scores - col_peak)
    col_total = lax.psum(jnp.sum(raw_weights, axis=0, keepdims=True), "seq")
    dispatch = raw_weights / col_total
    col_dot = lax.psum(jnp.sum(dispatch * weight_grad, axis=0, keepdims=True), "seq")
    logit_grad = (dispatch * (weight_grad - col_dot)).astype(jnp.bfloat16)
    dispatch_low = dispatch.astype(jnp.bfloat16)
    grad_scale = float(lax.axis_size("seq") * inputs.shape[0] // 16)
    token_sum = jnp.dot(dispatch_low, upstream, preferred_element_type=jnp.float32)
    token_sum = token_sum + lax.dot_general(
        logit_grad, phi_full, (((1,), (1,)), ((), ())), preferred_element_type=jnp.float32
    )
    token_grad = (grad_scale * token_sum).astype(jnp.bfloat16)[None]
    phi_terms = lax.dot_general(
        inputs, logit_grad, (((0,), (0,)), ((), ())), preferred_element_type=jnp.float32
    )
    phi_share = lax.psum_scatter(phi_terms, "seq", scatter_dimension=0, tiled=True)
    phi_grad = lax.psum(phi_share, "batch")
    return (token_grad, phi_grad)


def per_device(n, batches, tokens, logits, slot_grad, phi_param):
    own, slots = phi_param.shape
    if batches == 4 and n % 8 == 0 and slot_grad.shape[1] % 16 == 0 and own % 128 == 0 and slots % 128 == 0 and tokens.shape[1] % 256 == 0:
        token_grad, phi_grad = fused(n, tokens[0], logits[0], slot_grad[0], phi_param)
        return token_grad[None], phi_grad
    return plain(tokens, logits, slot_grad, phi_param)


def solution(mesh):
    return jax.shard_map(
        functools.partial(per_device, mesh.shape["seq"], mesh.shape["batch"]),
        mesh=mesh,
        in_specs=(
            P("batch", "seq", None),
            P("batch", "seq", None),
            P("batch", "seq", None),
            P("seq", None),
        ),
        out_specs=(P("batch", "seq", None), P("seq", None)),
        check_vma=False,
    )
```

```python
import functools

import jax
import jax.numpy as jnp
from jax import lax
from jax.experimental import pallas as pl
from jax.experimental.pallas import tpu as pltpu
from jax.sharding import PartitionSpec as P

MESH = pl.DeviceIdType.MESH
F32 = jnp.float32
BF16 = jnp.bfloat16


def fused_kernel(
    n, scale, tok_hbm, log_hbm, slot_hbm, phi_hbm, tok_out, phi_out,
    tok, log, raw, wg, gath, phig, stat, disp, lg, lgt, part, part_low, recv_a, sum_a, low_a,
    recv_b, sum_b, low_b, recv_c, fin,
    load_sem, ag_send, ag_recv, fw_send, fw_recv, st_send, st_recv, ph_send, ph_recv,
    pb_send, pb_recv, a_send, a_recv, b_send, b_recv, c_send, c_recv, d_send, d_recv,
):
    me = lax.axis_index("seq")
    bat = lax.axis_index("batch")
    half = n // 2
    twin = me + 1 - 2 * (me % 2)
    bat_a = bat + 1 - 2 * (bat % 2)
    bat_b = (bat + 2) % 4
    bat_c = (bat_a + 2) % 4
    keep_a = bat % 2
    keep_b = bat // 2
    rows = tok.shape[0]
    step = min(256, rows)
    steps = rows // step

    def remote(src, dst, send, recv, seq_at, bat_at):
        return pltpu.make_async_remote_copy(
            src_ref=src, dst_ref=dst, send_sem=send, recv_sem=recv,
            device_id=(seq_at, bat_at), device_id_type=MESH,
        )

    load_slot = pltpu.make_async_copy(slot_hbm, gath.at[me], load_sem.at[0])
    load_log = pltpu.make_async_copy(log_hbm, log, load_sem.at[1])
    load_phi = pltpu.make_async_copy(phi_hbm.at[bat], phig.at[me, bat], load_sem.at[2])
    load_tok = pltpu.make_async_copy(tok_hbm, tok, load_sem.at[3])
    load_slot.start()
    load_log.start()
    load_tok.start()
    load_phi.start()

    barrier = pltpu.get_barrier_semaphore()
    for k in range(1, n):
        pl.semaphore_signal(barrier, inc=1, device_id=((me + k) % n, bat), device_id_type=MESH)
    for other in (bat_a, bat_b, bat_c):
        pl.semaphore_signal(barrier, inc=1, device_id=(me, other), device_id_type=MESH)
    pl.semaphore_wait(barrier, n - 1 + 3)

    load_slot.wait()
    pieces = 2 if gath.shape[1] % 32 == 0 else 1
    piece = gath.shape[1] // pieces

    def shard(j, h):
        return gath.at[j, pl.ds(h * piece, piece)]

    to_twin = []
    direct = []
    for h in range(pieces):
        to_twin.append(remote(shard(me, h), shard(me, h), fw_send.at[0, h], fw_recv.at[0, h], twin, bat))
        to_twin[-1].start()
        for k in range(1, half):
            direct.append(remote(shard(me, h), shard(me, h), ag_send.at[k, h], ag_recv.at[k, h], (me + 2 * k) % n, bat))
            direct[-1].start()

    load_log.wait()

    def chunk(i):
        return pl.ds(pl.multiple_of(i * step, step), step)

    def peak_step(i, top):
        return jnp.maximum(top, jnp.max(log[chunk(i), :].astype(F32), axis=0, keepdims=True))

    slots = log.shape[1]
    peak = lax.fori_loop(0, steps, peak_step, jnp.full((1, slots), -jnp.inf, F32))

    def exp_step(i, acc):
        values = jnp.exp(log[chunk(i), :].astype(F32) - peak)
        raw[chunk(i), :] = values
        return acc + jnp.sum(values, axis=0, keepdims=True)

    total = lax.fori_loop(0, steps, exp_step, jnp.zeros((1, slots), F32))

    load_tok.wait()
    relayed = []
    for h in range(pieces):
        for k in range(1, half):
            source = (me - 2 * k + n) % n
            direct[h * (half - 1) + k - 1].wait_recv()
            relayed.append(remote(shard(source, h), shard(source, h), fw_send.at[k, h], fw_recv.at[k, h], twin, bat))
            relayed[-1].start()
    for move in to_twin + relayed:
        move.wait_recv()

    upstream = gath.reshape(slots, gath.shape[2])

    def wg_step(i, acc):
        values = lax.dot_general(
            tok[chunk(i), :], upstream[...], (((1,), (1,)), ((), ())), preferred_element_type=F32
        )
        wg[chunk(i), :] = values
        return acc + jnp.sum(values * raw[chunk(i), :], axis=0, keepdims=True)

    dot = lax.fori_loop(0, steps, wg_step, jnp.zeros((1, slots), F32))

    stat[me, 0:1, :] = peak
    stat[me, 1:2, :] = total
    stat[me, 2:3, :] = dot
    stat_moves = []
    for k in range(1, n):
        stat_moves.append(remote(stat.at[me], stat.at[me], st_send.at[k], st_recv.at[k], (me + k) % n, bat))
        stat_moves[-1].start()

    load_phi.wait()
    phi_moves = []
    for k in range(1, n):
        phi_moves.append(remote(phig.at[me, bat], phig.at[me, bat], ph_send.at[k], ph_recv.at[k], (me + k) % n, bat))
        phi_moves[-1].start()

    for move in stat_moves:
        move.wait_recv()
    peaks = stat[:, 0, :]
    col_peak = jnp.max(peaks, axis=0, keepdims=True)
    shifts = jnp.exp(peaks - col_peak)
    col_total = jnp.sum(stat[:, 1, :] * shifts, axis=0, keepdims=True)
    col_dot = jnp.sum(stat[:, 2, :] * shifts, axis=0, keepdims=True) / col_total
    factor = jnp.exp(peak - col_peak) / col_total

    def grad_step(i, carry):
        weights = raw[chunk(i), :] * factor
        grads = weights * (wg[chunk(i), :] - col_dot)
        disp[chunk(i), :] = weights.astype(BF16)
        lg[chunk(i), :] = grads.astype(BF16)
        lgt[:, chunk(i)] = grads.T.astype(BF16)
        return carry

    lax.fori_loop(0, steps, grad_step, 0)

    own = tok.shape[1] // n
    quarter = slots // 4

    group = n // 2
    owners = [[j for j in range(n) if (n // 4 <= j < n - n // 4) == bool(g)] for g in range(2)]
    moves_a = []
    for g in range(2):
        for at in range(0, group, 2):
            j = owners[g][at]
            terms = jnp.dot(lgt[...], tok[:, own * j : own * (j + 2)], preferred_element_type=F32)
            for side in range(2):
                for qa in range(2):
                    for qb in range(2):
                        first = (2 * qa + qb) * quarter
                        block = terms[first : first + quarter, side * own : (side + 1) * own]
                        part[g, qa, qb, at + side] = block
                        part_low[g, qa, qb, at + side] = block.astype(BF16)
        moves_a.append(remote(part_low.at[g, 1 - keep_a], recv_a.at[g], a_send.at[g], a_recv.at[g], me, bat_a))
        moves_a[-1].start()
    moves_b = []
    for g in range(2):
        moves_a[g].wait_recv()
        for qb in range(2):
            for at in range(group):
                block = part[g, keep_a, qb, at] + recv_a[g, qb, at].astype(F32)
                sum_a[g, qb, at] = block
                low_a[g, qb, at] = block.astype(BF16)
        moves_b.append(remote(low_a.at[g, 1 - keep_b], recv_b.at[g], b_send.at[g], b_recv.at[g], me, bat_b))
        moves_b[-1].start()
    for move in phi_moves:
        move.wait_recv()
    phi_b = remote(phig.at[:, bat], phig.at[:, bat], pb_send.at[0], pb_recv.at[0], me, bat_b)
    phi_b.start()

    def share_move(g, at):
        j = owners[g][at]
        return remote(low_b.at[g, at], recv_c.at[me], c_send.at[j], c_recv.at[me], j, bat)

    for g in range(2):
        moves_b[g].wait_recv()
        for at in range(group):
            block = sum_a[g, keep_b, at] + recv_b[g, at].astype(F32)
            sum_b[owners[g][at]] = block
            low_b[g, at] = block.astype(BF16)
        for at in range(group):
            @pl.when(me != owners[g][at])
            def _(g=g, at=at):
                share_move(g, at).start()

    phi_b.wait_recv()
    phi_a = [
        remote(phig.at[:, bat], phig.at[:, bat], pb_send.at[1], pb_recv.at[1], me, bat_a),
        remote(phig.at[:, bat_b], phig.at[:, bat_b], pb_send.at[2], pb_recv.at[2], me, bat_a),
    ]
    for move in phi_a:
        move.start()
    share = sum_b[me]
    for k in range(1, n):
        source = (me - k + n) % n
        remote(low_b.at[0, 0], recv_c.at[source], c_send.at[0], c_recv.at[source], source, bat).wait_recv()
        share = share + recv_c[source].astype(F32)
    mine = 2 * keep_a + keep_b
    fin[mine] = share
    last = []
    for k, other in enumerate((bat_c, bat_b, bat_a)):
        last.append(remote(fin.at[mine], fin.at[mine], d_send.at[k], d_recv.at[k], me, other))
        last[-1].start()
    for move in phi_a:
        move.wait_recv()

    phi_full = phig.reshape(phig.shape[0] * phig.shape[1] * phig.shape[2], phig.shape[3])

    def out_step(i, carry):
        values = jnp.dot(disp[chunk(i), :], upstream[...], preferred_element_type=F32)
        values = values + lax.dot_general(
            lg[chunk(i), :], phi_full[...], (((1,), (1,)), ((), ())), preferred_element_type=F32
        )
        tok_out[chunk(i), :] = (scale * values).astype(BF16)
        return carry

    lax.fori_loop(0, steps, out_step, 0)

    for move in last:
        move.wait_recv()
    phi_out[...] = fin[...].reshape(slots, own).T

    for g in range(2):
        for at in range(group):
            @pl.when(me != owners[g][at])
            def _(g=g, at=at):
                share_move(g, at).wait_send()
    for move in to_twin + direct + relayed + stat_moves + phi_moves + moves_a + moves_b + [phi_b] + phi_a + last:
        move.wait_send()


def fused(n, tokens, logits, slot_grad, phi_param):
    rows, width = tokens.shape
    slots = logits.shape[1]
    own = width // n
    quarter = slots // 4
    scale = float(n * rows // 16)
    dma = pltpu.SemaphoreType.DMA
    hbm = pl.BlockSpec(memory_space=pltpu.HBM)
    return pl.pallas_call(
        functools.partial(fused_kernel, n, scale),
        out_shape=(
            jax.ShapeDtypeStruct((rows, width), BF16),
            jax.ShapeDtypeStruct((own, slots), F32),
        ),
        in_specs=[hbm] * 4,
        out_specs=(pl.BlockSpec(memory_space=pltpu.VMEM), pl.BlockSpec(memory_space=pltpu.VMEM)),
        scratch_shapes=[
            pltpu.VMEM((rows, width), BF16),
            pltpu.VMEM((rows, slots), BF16),
            pltpu.VMEM((rows, slots), F32),
            pltpu.VMEM((rows, slots), F32),
            pltpu.VMEM((n, slots // n, width), BF16),
            pltpu.VMEM((n, 4, own // 4, slots), BF16),
            pltpu.VMEM((n, 8, slots), F32),
            pltpu.VMEM((rows, slots), BF16),
            pltpu.VMEM((rows, slots), BF16),
            pltpu.VMEM((slots, rows), BF16),
            pltpu.VMEM((2, 2, 2, n // 2, quarter, own), F32),
            pltpu.VMEM((2, 2, 2, n // 2, quarter, own), BF16),
            pltpu.VMEM((2, 2, n // 2, quarter, own), BF16),
            pltpu.VMEM((2, 2, n // 2, quarter, own), F32),
            pltpu.VMEM((2, 2, n // 2, quarter, own), BF16),
            pltpu.VMEM((2, n // 2, quarter, own), BF16),
            pltpu.VMEM((n, quarter, own), F32),
            pltpu.VMEM((2, n // 2, quarter, own), BF16),
            pltpu.VMEM((n, quarter, own), BF16),
            pltpu.VMEM((4, quarter, own), F32),
            dma((4,)),
            dma((n // 2, 2)), dma((n // 2, 2)),
            dma((n // 2, 2)), dma((n // 2, 2)),
            dma((n,)), dma((n,)),
            dma((n,)), dma((n,)),
            dma((3,)), dma((3,)),
            dma((2,)), dma((2,)),
            dma((2,)), dma((2,)),
            dma((n,)), dma((n,)),
            dma((3,)), dma((3,)),
        ],
        compiler_params=pltpu.CompilerParams(
            collective_id=0, has_side_effects=True, vmem_limit_bytes=52_000_000
        ),
    )(*[
        pltpu.with_memory_space_constraint(x, pltpu.HBM)
        for x in (tokens, logits, slot_grad, phi_param.reshape(4, own // 4, slots))
    ])


def plain(tokens, logits, slot_grad, phi_param):
    inputs = tokens[0]
    scores = logits[0].astype(jnp.float32)
    upstream, phi_full = (
        lax.all_gather(slot_grad[0], "seq", axis=0, tiled=True),
        lax.all_gather(phi_param, "seq", axis=0, tiled=True),
    )
    weight_grad = lax.dot_general(
        inputs, upstream, (((1,), (1,)), ((), ())), preferred_element_type=jnp.float32
    )
    col_peak = lax.pmax(jnp.max(scores, axis=0, keepdims=True), "seq")
    raw_weights = jnp.exp(scores - col_peak)
    col_total = lax.psum(jnp.sum(raw_weights, axis=0, keepdims=True), "seq")
    dispatch = raw_weights / col_total
    col_dot = lax.psum(jnp.sum(dispatch * weight_grad, axis=0, keepdims=True), "seq")
    logit_grad = (dispatch * (weight_grad - col_dot)).astype(jnp.bfloat16)
    dispatch_low = dispatch.astype(jnp.bfloat16)
    grad_scale = float(lax.axis_size("seq") * inputs.shape[0] // 16)
    token_sum = jnp.dot(dispatch_low, upstream, preferred_element_type=jnp.float32)
    token_sum = token_sum + lax.dot_general(
        logit_grad, phi_full, (((1,), (1,)), ((), ())), preferred_element_type=jnp.float32
    )
    token_grad = (grad_scale * token_sum).astype(jnp.bfloat16)[None]
    phi_terms = lax.dot_general(
        inputs, logit_grad, (((0,), (0,)), ((), ())), preferred_element_type=jnp.float32
    )
    phi_share = lax.psum_scatter(phi_terms, "seq", scatter_dimension=0, tiled=True)
    phi_grad = lax.psum(phi_share, "batch")
    return (token_grad, phi_grad)


def per_device(n, batches, tokens, logits, slot_grad, phi_param):
    own, slots = phi_param.shape
    if batches == 4 and n % 8 == 0 and slot_grad.shape[1] % 16 == 0 and own % 128 == 0 and slots % 128 == 0 and tokens.shape[1] % 256 == 0:
        token_grad, phi_grad = fused(n, tokens[0], logits[0], slot_grad[0], phi_param)
        return token_grad[None], phi_grad
    return plain(tokens, logits, slot_grad, phi_param)


def solution(mesh):
    return jax.shard_map(
        functools.partial(per_device, mesh.shape["seq"], mesh.shape["batch"]),
        mesh=mesh,
        in_specs=(
            P("batch", "seq", None),
            P("batch", "seq", None),
            P("batch", "seq", None),
            P("seq", None),
        ),
        out_specs=(P("batch", "seq", None), P("seq", None)),
        check_vma=False,
    )
```

```python
import functools

import jax
import jax.numpy as jnp
from jax import lax
from jax.experimental import pallas as pl
from jax.experimental.pallas import tpu as pltpu
from jax.sharding import PartitionSpec as P

MESH = pl.DeviceIdType.MESH
F32 = jnp.float32
BF16 = jnp.bfloat16


def fused_kernel(
    n, scale, tok_hbm, log_hbm, slot_hbm, phi_hbm, tok_out, phi_out,
    tok, log, raw, wg, gath, phig, stat, disp, lg, lgt, part, part_low, recv_a, sum_a, low_a,
    recv_b, sum_b, low_b, recv_c, fin,
    load_sem, ag_send, ag_recv, fw_send, fw_recv, st_send, st_recv, ph_send, ph_recv,
    pb_send, pb_recv, a_send, a_recv, b_send, b_recv, c_send, c_recv, d_send, d_recv,
):
    me = lax.axis_index("seq")
    bat = lax.axis_index("batch")
    half = n // 2
    twin = me + 1 - 2 * (me % 2)
    bat_a = bat + 1 - 2 * (bat % 2)
    bat_b = (bat + 2) % 4
    bat_c = (bat_a + 2) % 4
    keep_a = bat % 2
    keep_b = bat // 2
    rows = tok.shape[0]
    step = min(256, rows)
    steps = rows // step

    def remote(src, dst, send, recv, seq_at, bat_at):
        return pltpu.make_async_remote_copy(
            src_ref=src, dst_ref=dst, send_sem=send, recv_sem=recv,
            device_id=(seq_at, bat_at), device_id_type=MESH,
        )

    load_slot = pltpu.make_async_copy(slot_hbm, gath.at[me], load_sem.at[0])
    load_log = pltpu.make_async_copy(log_hbm, log, load_sem.at[1])
    load_phi = pltpu.make_async_copy(phi_hbm.at[bat], phig.at[me, bat], load_sem.at[2])
    load_tok = pltpu.make_async_copy(tok_hbm, tok, load_sem.at[3])
    load_slot.start()
    load_log.start()
    load_tok.start()
    load_phi.start()

    barrier = pltpu.get_barrier_semaphore()
    for k in range(1, n):
        pl.semaphore_signal(barrier, inc=1, device_id=((me + k) % n, bat), device_id_type=MESH)
    for other in (bat_a, bat_b, bat_c):
        pl.semaphore_signal(barrier, inc=1, device_id=(me, other), device_id_type=MESH)
    pl.semaphore_wait(barrier, n - 1 + 3)

    load_slot.wait()
    pieces = 2 if gath.shape[1] % 32 == 0 else 1
    piece = gath.shape[1] // pieces

    def shard(j, h):
        return gath.at[j, pl.ds(h * piece, piece)]

    place = me // 2
    low = 1 - place // (half // 2)

    def column_peer(i):
        at = low * (half - 1 - i) + (1 - low) * i
        return at - low * ((place - at + half) // half) + (1 - low) * ((at - place + half) // half)

    to_twin = []
    direct = []
    for h in range(pieces):
        to_twin.append(remote(shard(me, h), shard(me, h), fw_send.at[0, h], fw_recv.at[me // 2, h], twin, bat))
        to_twin[-1].start()
        for k in range(1, half):
            target = column_peer(k - 1)
            direct.append(remote(
                shard(me, h), shard(me, h), ag_send.at[k, h], ag_recv.at[me // 2, h], 2 * target + me % 2, bat))
            direct[-1].start()

    load_log.wait()

    def chunk(i):
        return pl.ds(pl.multiple_of(i * step, step), step)

    def peak_step(i, top):
        return jnp.maximum(top, jnp.max(log[chunk(i), :].astype(F32), axis=0, keepdims=True))

    slots = log.shape[1]
    peak = lax.fori_loop(0, steps, peak_step, jnp.full((1, slots), -jnp.inf, F32))

    def exp_step(i, acc):
        values = jnp.exp(log[chunk(i), :].astype(F32) - peak)
        raw[chunk(i), :] = values
        return acc + jnp.sum(values, axis=0, keepdims=True)

    total = lax.fori_loop(0, steps, exp_step, jnp.zeros((1, slots), F32))

    load_tok.wait()
    relayed = []
    for h in range(pieces):
        for k in range(1, half):
            origin = column_peer(k - 1)
            source = 2 * origin + me % 2
            remote(shard(source, h), shard(source, h), ag_send.at[k, h], ag_recv.at[origin, h], source, bat).wait_recv()
            relayed.append(
                remote(shard(source, h), shard(source, h), fw_send.at[k, h], fw_recv.at[origin, h], twin, bat))
            relayed[-1].start()
    for h in range(pieces):
        for j in range(half):
            source = 2 * j + twin % 2
            remote(shard(source, h), shard(source, h), fw_send.at[0, h], fw_recv.at[j, h], twin, bat).wait_recv()

    upstream = gath.reshape(slots, gath.shape[2])

    large = 2 * step if rows % (2 * step) == 0 else step

    def wide(i):
        return pl.ds(pl.multiple_of(i * large, large), large)

    def wg_step(i, acc):
        values = lax.dot_general(
            tok[wide(i), :], upstream[...], (((1,), (1,)), ((), ())), preferred_element_type=F32
        )
        wg[wide(i), :] = values
        return acc + jnp.sum(values * raw[wide(i), :], axis=0, keepdims=True)

    dot = lax.fori_loop(0, rows // large, wg_step, jnp.zeros((1, slots), F32))

    stat[me, 0:1, :] = peak
    stat[me, 1:2, :] = total
    stat[me, 2:3, :] = dot
    stat_moves = []
    for k in range(1, n):
        stat_moves.append(remote(stat.at[me], stat.at[me], st_send.at[k], st_recv.at[k], (me + k) % n, bat))
        stat_moves[-1].start()

    load_phi.wait()
    phi_moves = []
    for k in range(1, n):
        phi_moves.append(remote(phig.at[me, bat], phig.at[me, bat], ph_send.at[k], ph_recv.at[k], (me + k) % n, bat))
        phi_moves[-1].start()

    for move in stat_moves:
        move.wait_recv()
    peaks = stat[:, 0, :]
    col_peak = jnp.max(peaks, axis=0, keepdims=True)
    shifts = jnp.exp(peaks - col_peak)
    col_total = jnp.sum(stat[:, 1, :] * shifts, axis=0, keepdims=True)
    col_dot = jnp.sum(stat[:, 2, :] * shifts, axis=0, keepdims=True) / col_total
    factor = jnp.exp(peak - col_peak) / col_total

    def grad_step(i, carry):
        weights = raw[chunk(i), :] * factor
        grads = weights * (wg[chunk(i), :] - col_dot)
        disp[chunk(i), :] = weights.astype(BF16)
        lg[chunk(i), :] = grads.astype(BF16)
        lgt[:, chunk(i)] = grads.T.astype(BF16)
        return carry

    lax.fori_loop(0, steps, grad_step, 0)

    own = tok.shape[1] // n
    quarter = slots // 4

    group = n // 2
    owners = [[j for j in range(n) if (n // 4 <= j < n - n // 4) == bool(g)] for g in range(2)]
    moves_a = []
    for g in range(2):
        for at in range(0, group, 2):
            j = owners[g][at]
            terms = jnp.dot(lgt[...], tok[:, own * j : own * (j + 2)], preferred_element_type=F32)
            for side in range(2):
                for qa in range(2):
                    for qb in range(2):
                        first = (2 * qa + qb) * quarter
                        block = terms[first : first + quarter, side * own : (side + 1) * own]
                        part[g, qa, qb, at + side] = block
                        part_low[g, qa, qb, at + side] = block.astype(BF16)
        moves_a.append(remote(part_low.at[g, 1 - keep_a], recv_a.at[g], a_send.at[g], a_recv.at[g], me, bat_a))
        moves_a[-1].start()
    moves_b = []
    for g in range(2):
        moves_a[g].wait_recv()
        for qb in range(2):
            for at in range(group):
                block = part[g, keep_a, qb, at] + recv_a[g, qb, at].astype(F32)
                sum_a[g, qb, at] = block
                low_a[g, qb, at] = block.astype(BF16)
        moves_b.append(remote(low_a.at[g, 1 - keep_b], recv_b.at[g], b_send.at[g], b_recv.at[g], me, bat_b))
        moves_b[-1].start()
    for move in phi_moves:
        move.wait_recv()
    phi_b = remote(phig.at[:, bat], phig.at[:, bat], pb_send.at[0], pb_recv.at[0], me, bat_b)
    phi_b.start()

    def share_move(g, at):
        j = owners[g][at]
        return remote(low_b.at[g, at], recv_c.at[me], c_send.at[j], c_recv.at[me], j, bat)

    for g in range(2):
        moves_b[g].wait_recv()
        for at in range(group):
            block = sum_a[g, keep_b, at] + recv_b[g, at].astype(F32)
            sum_b[owners[g][at]] = block
            low_b[g, at] = block.astype(BF16)
        for at in range(group):
            @pl.when(me != owners[g][at])
            def _(g=g, at=at):
                share_move(g, at).start()

    phi_b.wait_recv()
    phi_a = [
        remote(phig.at[:, bat], phig.at[:, bat], pb_send.at[1], pb_recv.at[1], me, bat_a),
        remote(phig.at[:, bat_b], phig.at[:, bat_b], pb_send.at[2], pb_recv.at[2], me, bat_a),
    ]
    for move in phi_a:
        move.start()
    share = sum_b[me]
    for k in range(1, n):
        source = (me - k + n) % n
        remote(low_b.at[0, 0], recv_c.at[source], c_send.at[0], c_recv.at[source], source, bat).wait_recv()
        share = share + recv_c[source].astype(F32)
    mine = 2 * keep_a + keep_b
    fin[mine] = share
    last = []
    for k, other in enumerate((bat_c, bat_b, bat_a)):
        last.append(remote(fin.at[mine], fin.at[mine], d_send.at[k], d_recv.at[k], me, other))
        last[-1].start()
    for move in phi_a:
        move.wait_recv()

    phi_full = phig.reshape(phig.shape[0] * phig.shape[1] * phig.shape[2], phig.shape[3])

    def out_step(i, carry):
        values = jnp.dot(disp[wide(i), :], upstream[...], preferred_element_type=F32)
        values = values + lax.dot_general(
            lg[wide(i), :], phi_full[...], (((1,), (1,)), ((), ())), preferred_element_type=F32
        )
        tok_out[wide(i), :] = (scale * values).astype(BF16)
        return carry

    lax.fori_loop(0, rows // large, out_step, 0)

    for move in last:
        move.wait_recv()
    phi_out[...] = fin[...].reshape(slots, own).T

    for g in range(2):
        for at in range(group):
            @pl.when(me != owners[g][at])
            def _(g=g, at=at):
                share_move(g, at).wait_send()
    for move in to_twin + direct + relayed + stat_moves + phi_moves + moves_a + moves_b + [phi_b] + phi_a + last:
        move.wait_send()


def fused(n, tokens, logits, slot_grad, phi_param):
    rows, width = tokens.shape
    slots = logits.shape[1]
    own = width // n
    quarter = slots // 4
    scale = float(n * rows // 16)
    dma = pltpu.SemaphoreType.DMA
    hbm = pl.BlockSpec(memory_space=pltpu.HBM)
    return pl.pallas_call(
        functools.partial(fused_kernel, n, scale),
        out_shape=(
            jax.ShapeDtypeStruct((rows, width), BF16),
            jax.ShapeDtypeStruct((own, slots), F32),
        ),
        in_specs=[hbm] * 4,
        out_specs=(pl.BlockSpec(memory_space=pltpu.VMEM), pl.BlockSpec(memory_space=pltpu.VMEM)),
        scratch_shapes=[
            pltpu.VMEM((rows, width), BF16),
            pltpu.VMEM((rows, slots), BF16),
            pltpu.VMEM((rows, slots), F32),
            pltpu.VMEM((rows, slots), F32),
            pltpu.VMEM((n, slots // n, width), BF16),
            pltpu.VMEM((n, 4, own // 4, slots), BF16),
            pltpu.VMEM((n, 8, slots), F32),
            pltpu.VMEM((rows, slots), BF16),
            pltpu.VMEM((rows, slots), BF16),
            pltpu.VMEM((slots, rows), BF16),
            pltpu.VMEM((2, 2, 2, n // 2, quarter, own), F32),
            pltpu.VMEM((2, 2, 2, n // 2, quarter, own), BF16),
            pltpu.VMEM((2, 2, n // 2, quarter, own), BF16),
            pltpu.VMEM((2, 2, n // 2, quarter, own), F32),
            pltpu.VMEM((2, 2, n // 2, quarter, own), BF16),
            pltpu.VMEM((2, n // 2, quarter, own), BF16),
            pltpu.VMEM((n, quarter, own), F32),
            pltpu.VMEM((2, n // 2, quarter, own), BF16),
            pltpu.VMEM((n, quarter, own), BF16),
            pltpu.VMEM((4, quarter, own), F32),
            dma((4,)),
            dma((n // 2, 2)), dma((n // 2, 2)),
            dma((n // 2, 2)), dma((n // 2, 2)),
            dma((n,)), dma((n,)),
            dma((n,)), dma((n,)),
            dma((3,)), dma((3,)),
            dma((2,)), dma((2,)),
            dma((2,)), dma((2,)),
            dma((n,)), dma((n,)),
            dma((3,)), dma((3,)),
        ],
        compiler_params=pltpu.CompilerParams(
            collective_id=0, has_side_effects=True, vmem_limit_bytes=52_000_000
        ),
    )(*[
        pltpu.with_memory_space_constraint(x, pltpu.HBM)
        for x in (tokens, logits, slot_grad, phi_param.reshape(4, own // 4, slots))
    ])


def plain(tokens, logits, slot_grad, phi_param):
    inputs = tokens[0]
    scores = logits[0].astype(jnp.float32)
    upstream, phi_full = (
        lax.all_gather(slot_grad[0], "seq", axis=0, tiled=True),
        lax.all_gather(phi_param, "seq", axis=0, tiled=True),
    )
    weight_grad = lax.dot_general(
        inputs, upstream, (((1,), (1,)), ((), ())), preferred_element_type=jnp.float32
    )
    col_peak = lax.pmax(jnp.max(scores, axis=0, keepdims=True), "seq")
    raw_weights = jnp.exp(scores - col_peak)
    col_total = lax.psum(jnp.sum(raw_weights, axis=0, keepdims=True), "seq")
    dispatch = raw_weights / col_total
    col_dot = lax.psum(jnp.sum(dispatch * weight_grad, axis=0, keepdims=True), "seq")
    logit_grad = (dispatch * (weight_grad - col_dot)).astype(jnp.bfloat16)
    dispatch_low = dispatch.astype(jnp.bfloat16)
    grad_scale = float(lax.axis_size("seq") * inputs.shape[0] // 16)
    token_sum = jnp.dot(dispatch_low, upstream, preferred_element_type=jnp.float32)
    token_sum = token_sum + lax.dot_general(
        logit_grad, phi_full, (((1,), (1,)), ((), ())), preferred_element_type=jnp.float32
    )
    token_grad = (grad_scale * token_sum).astype(jnp.bfloat16)[None]
    phi_terms = lax.dot_general(
        inputs, logit_grad, (((0,), (0,)), ((), ())), preferred_element_type=jnp.float32
    )
    phi_share = lax.psum_scatter(phi_terms, "seq", scatter_dimension=0, tiled=True)
    phi_grad = lax.psum(phi_share, "batch")
    return (token_grad, phi_grad)


def per_device(n, batches, tokens, logits, slot_grad, phi_param):
    own, slots = phi_param.shape
    if batches == 4 and n % 8 == 0 and slot_grad.shape[1] % 16 == 0 and own % 128 == 0 and slots % 128 == 0 and tokens.shape[1] % 256 == 0:
        token_grad, phi_grad = fused(n, tokens[0], logits[0], slot_grad[0], phi_param)
        return token_grad[None], phi_grad
    return plain(tokens, logits, slot_grad, phi_param)


def solution(mesh):
    return jax.shard_map(
        functools.partial(per_device, mesh.shape["seq"], mesh.shape["batch"]),
        mesh=mesh,
        in_specs=(
            P("batch", "seq", None),
            P("batch", "seq", None),
            P("batch", "seq", None),
            P("seq", None),
        ),
        out_specs=(P("batch", "seq", None), P("seq", None)),
        check_vma=False,
    )
```

```python
import functools

import jax
import jax.numpy as jnp
from jax import lax
from jax.experimental import pallas as pl
from jax.experimental.pallas import tpu as pltpu
from jax.sharding import PartitionSpec as P

MESH = pl.DeviceIdType.MESH
F32 = jnp.float32
BF16 = jnp.bfloat16


def fused_kernel(
    n, scale, tok_hbm, log_hbm, slot_hbm, phi_hbm, tok_out, phi_out,
    tok, log, raw, wg, gath, phig, stat, disp, lg, tokt, part, part_low, recv_a, sum_a, low_a,
    recv_b, sum_b, low_b, recv_c, fin,
    load_sem, ag_send, ag_recv, fw_send, fw_recv, st_send, st_recv, ph_send, ph_recv,
    pb_send, pb_recv, a_send, a_recv, b_send, b_recv, c_send, c_recv, d_send, d_recv,
):
    me = lax.axis_index("seq")
    bat = lax.axis_index("batch")
    half = n // 2
    twin = me + 1 - 2 * (me % 2)
    bat_a = bat + 1 - 2 * (bat % 2)
    bat_b = (bat + 2) % 4
    bat_c = (bat_a + 2) % 4
    keep_a = bat % 2
    keep_b = bat // 2
    rows = tok.shape[0]
    step = min(256, rows)
    steps = rows // step

    def remote(src, dst, send, recv, seq_at, bat_at):
        return pltpu.make_async_remote_copy(
            src_ref=src, dst_ref=dst, send_sem=send, recv_sem=recv,
            device_id=(seq_at, bat_at), device_id_type=MESH,
        )

    load_slot = pltpu.make_async_copy(slot_hbm, gath.at[me], load_sem.at[0])
    load_log = pltpu.make_async_copy(log_hbm, log, load_sem.at[1])
    load_phi = pltpu.make_async_copy(phi_hbm.at[bat], phig.at[me, bat], load_sem.at[2])
    load_tok = pltpu.make_async_copy(tok_hbm, tok, load_sem.at[3])
    load_slot.start()
    load_log.start()
    load_tok.start()
    load_phi.start()

    barrier = pltpu.get_barrier_semaphore()
    for k in range(1, n):
        pl.semaphore_signal(barrier, inc=1, device_id=((me + k) % n, bat), device_id_type=MESH)
    for other in (bat_a, bat_b, bat_c):
        pl.semaphore_signal(barrier, inc=1, device_id=(me, other), device_id_type=MESH)
    pl.semaphore_wait(barrier, n - 1 + 3)

    load_slot.wait()
    pieces = 2 if gath.shape[1] % 32 == 0 else 1
    piece = gath.shape[1] // pieces

    def shard(j, h):
        return gath.at[j, pl.ds(h * piece, piece)]

    place = me // 2
    low = 1 - place // (half // 2)

    def column_peer(i):
        at = low * (half - 1 - i) + (1 - low) * i
        return at - low * ((place - at + half) // half) + (1 - low) * ((at - place + half) // half)

    to_twin = []
    direct = []
    for h in range(pieces):
        to_twin.append(remote(shard(me, h), shard(me, h), fw_send.at[0, h], fw_recv.at[me // 2, h], twin, bat))
        to_twin[-1].start()
        for k in range(1, half):
            target = column_peer(k - 1)
            direct.append(remote(
                shard(me, h), shard(me, h), ag_send.at[k, h], ag_recv.at[me // 2, h], 2 * target + me % 2, bat))
            direct[-1].start()

    load_log.wait()

    def chunk(i):
        return pl.ds(pl.multiple_of(i * step, step), step)

    def peak_step(i, top):
        return jnp.maximum(top, jnp.max(log[chunk(i), :].astype(F32), axis=0, keepdims=True))

    slots = log.shape[1]
    peak = lax.fori_loop(0, steps, peak_step, jnp.full((1, slots), -jnp.inf, F32))

    def exp_step(i, acc):
        values = jnp.exp(log[chunk(i), :].astype(F32) - peak)
        raw[chunk(i), :] = values
        return acc + jnp.sum(values, axis=0, keepdims=True)

    total = lax.fori_loop(0, steps, exp_step, jnp.zeros((1, slots), F32))

    load_tok.wait()

    def turn_step(i, carry):
        tokt[:, chunk(i)] = tok[chunk(i), :].T
        return carry

    lax.fori_loop(0, steps, turn_step, 0)
    relayed = []
    for h in range(pieces):
        for k in range(1, half):
            origin = column_peer(k - 1)
            source = 2 * origin + me % 2
            remote(shard(source, h), shard(source, h), ag_send.at[k, h], ag_recv.at[origin, h], source, bat).wait_recv()
            relayed.append(
                remote(shard(source, h), shard(source, h), fw_send.at[k, h], fw_recv.at[origin, h], twin, bat))
            relayed[-1].start()
    for h in range(pieces):
        for j in range(half):
            source = 2 * j + twin % 2
            remote(shard(source, h), shard(source, h), fw_send.at[0, h], fw_recv.at[j, h], twin, bat).wait_recv()

    upstream = gath.reshape(slots, gath.shape[2])

    large = 2 * step if rows % (2 * step) == 0 else step

    def wide(i):
        return pl.ds(pl.multiple_of(i * large, large), large)

    def wg_step(i, acc):
        values = lax.dot_general(
            tok[wide(i), :], upstream[...], (((1,), (1,)), ((), ())), preferred_element_type=F32
        )
        wg[wide(i), :] = values
        return acc + jnp.sum(values * raw[wide(i), :], axis=0, keepdims=True)

    dot = lax.fori_loop(0, rows // large, wg_step, jnp.zeros((1, slots), F32))

    stat[me, 0:1, :] = peak
    stat[me, 1:2, :] = total
    stat[me, 2:3, :] = dot
    stat_moves = []
    for k in range(1, n):
        stat_moves.append(remote(stat.at[me], stat.at[me], st_send.at[k], st_recv.at[k], (me + k) % n, bat))
        stat_moves[-1].start()

    load_phi.wait()
    phi_moves = []
    for k in range(1, n):
        phi_moves.append(remote(phig.at[me, bat], phig.at[me, bat], ph_send.at[k], ph_recv.at[k], (me + k) % n, bat))
        phi_moves[-1].start()

    for move in stat_moves:
        move.wait_recv()
    peaks = stat[:, 0, :]
    col_peak = jnp.max(peaks, axis=0, keepdims=True)
    shifts = jnp.exp(peaks - col_peak)
    col_total = jnp.sum(stat[:, 1, :] * shifts, axis=0, keepdims=True)
    col_dot = jnp.sum(stat[:, 2, :] * shifts, axis=0, keepdims=True) / col_total
    factor = jnp.exp(peak - col_peak) / col_total

    def grad_step(i, carry):
        weights = raw[chunk(i), :] * factor
        grads = weights * (wg[chunk(i), :] - col_dot)
        disp[chunk(i), :] = weights.astype(BF16)
        lg[chunk(i), :] = grads.astype(BF16)
        return carry

    lax.fori_loop(0, steps, grad_step, 0)

    own = tok.shape[1] // n
    quarter = own // 4

    group = n // 2
    owners = [[j for j in range(n) if (n // 4 <= j < n - n // 4) == bool(g)] for g in range(2)]
    moves_a = []
    for g in range(2):
        for at in range(0, group, 2):
            j = owners[g][at]
            terms = jnp.dot(tokt[own * j : own * (j + 2), :], lg[...], preferred_element_type=F32)
            for side in range(2):
                for qa in range(2):
                    for qb in range(2):
                        first = own * side + (2 * qa + qb) * quarter
                        block = terms[first : first + quarter, :]
                        part[g, qa, qb, at + side] = block
                        part_low[g, qa, qb, at + side] = block.astype(BF16)
        moves_a.append(remote(part_low.at[g, 1 - keep_a], recv_a.at[g], a_send.at[g], a_recv.at[g], me, bat_a))
        moves_a[-1].start()
    moves_b = []
    for g in range(2):
        moves_a[g].wait_recv()
        for qb in range(2):
            for at in range(group):
                block = part[g, keep_a, qb, at] + recv_a[g, qb, at].astype(F32)
                sum_a[g, qb, at] = block
                low_a[g, qb, at] = block.astype(BF16)
        moves_b.append(remote(low_a.at[g, 1 - keep_b], recv_b.at[g], b_send.at[g], b_recv.at[g], me, bat_b))
        moves_b[-1].start()
    for move in phi_moves:
        move.wait_recv()
    phi_b = remote(phig.at[:, bat], phig.at[:, bat], pb_send.at[0], pb_recv.at[0], me, bat_b)
    phi_b.start()

    def share_move(g, at):
        j = owners[g][at]
        return remote(low_b.at[g, at], recv_c.at[me], c_send.at[j], c_recv.at[me], j, bat)

    for g in range(2):
        moves_b[g].wait_recv()
        for at in range(group):
            block = sum_a[g, keep_b, at] + recv_b[g, at].astype(F32)
            sum_b[owners[g][at]] = block
            low_b[g, at] = block.astype(BF16)
        for at in range(group):
            @pl.when(me != owners[g][at])
            def _(g=g, at=at):
                share_move(g, at).start()

    phi_b.wait_recv()
    phi_a = [
        remote(phig.at[:, bat], phig.at[:, bat], pb_send.at[1], pb_recv.at[1], me, bat_a),
        remote(phig.at[:, bat_b], phig.at[:, bat_b], pb_send.at[2], pb_recv.at[2], me, bat_a),
    ]
    for move in phi_a:
        move.start()
    share = sum_b[me]
    for k in range(1, n):
        source = (me - k + n) % n
        remote(low_b.at[0, 0], recv_c.at[source], c_send.at[0], c_recv.at[source], source, bat).wait_recv()
        share = share + recv_c[source].astype(F32)
    mine = 2 * keep_a + keep_b
    fin[mine] = share
    last = []
    for k, other in enumerate((bat_c, bat_b, bat_a)):
        last.append(remote(fin.at[mine], fin.at[mine], d_send.at[k], d_recv.at[k], me, other))
        last[-1].start()
    for move in phi_a:
        move.wait_recv()

    phi_full = phig.reshape(phig.shape[0] * phig.shape[1] * phig.shape[2], phig.shape[3])

    def out_step(i, carry):
        values = jnp.dot(disp[wide(i), :], upstream[...], preferred_element_type=F32)
        values = values + lax.dot_general(
            lg[wide(i), :], phi_full[...], (((1,), (1,)), ((), ())), preferred_element_type=F32
        )
        tok_out[wide(i), :] = (scale * values).astype(BF16)
        return carry

    lax.fori_loop(0, rows // large, out_step, 0)

    for move in last:
        move.wait_recv()
    phi_out[...] = fin[...].reshape(own, slots)

    for g in range(2):
        for at in range(group):
            @pl.when(me != owners[g][at])
            def _(g=g, at=at):
                share_move(g, at).wait_send()
    for move in to_twin + direct + relayed + stat_moves + phi_moves + moves_a + moves_b + [phi_b] + phi_a + last:
        move.wait_send()


def fused(n, tokens, logits, slot_grad, phi_param):
    rows, width = tokens.shape
    slots = logits.shape[1]
    own = width // n
    scale = float(n * rows // 16)
    dma = pltpu.SemaphoreType.DMA
    hbm = pl.BlockSpec(memory_space=pltpu.HBM)
    return pl.pallas_call(
        functools.partial(fused_kernel, n, scale),
        out_shape=(
            jax.ShapeDtypeStruct((rows, width), BF16),
            jax.ShapeDtypeStruct((own, slots), F32),
        ),
        in_specs=[hbm] * 4,
        out_specs=(pl.BlockSpec(memory_space=pltpu.VMEM), pl.BlockSpec(memory_space=pltpu.VMEM)),
        scratch_shapes=[
            pltpu.VMEM((rows, width), BF16),
            pltpu.VMEM((rows, slots), BF16),
            pltpu.VMEM((rows, slots), F32),
            pltpu.VMEM((rows, slots), F32),
            pltpu.VMEM((n, slots // n, width), BF16),
            pltpu.VMEM((n, 4, own // 4, slots), BF16),
            pltpu.VMEM((n, 8, slots), F32),
            pltpu.VMEM((rows, slots), BF16),
            pltpu.VMEM((rows, slots), BF16),
            pltpu.VMEM((width, rows), BF16),
            pltpu.VMEM((2, 2, 2, n // 2, own // 4, slots), F32),
            pltpu.VMEM((2, 2, 2, n // 2, own // 4, slots), BF16),
            pltpu.VMEM((2, 2, n // 2, own // 4, slots), BF16),
            pltpu.VMEM((2, 2, n // 2, own // 4, slots), F32),
            pltpu.VMEM((2, 2, n // 2, own // 4, slots), BF16),
            pltpu.VMEM((2, n // 2, own // 4, slots), BF16),
            pltpu.VMEM((n, own // 4, slots), F32),
            pltpu.VMEM((2, n // 2, own // 4, slots), BF16),
            pltpu.VMEM((n, own // 4, slots), BF16),
            pltpu.VMEM((4, own // 4, slots), F32),
            dma((4,)),
            dma((n // 2, 2)), dma((n // 2, 2)),
            dma((n // 2, 2)), dma((n // 2, 2)),
            dma((n,)), dma((n,)),
            dma((n,)), dma((n,)),
            dma((3,)), dma((3,)),
            dma((2,)), dma((2,)),
            dma((2,)), dma((2,)),
            dma((n,)), dma((n,)),
            dma((3,)), dma((3,)),
        ],
        compiler_params=pltpu.CompilerParams(
            collective_id=0, has_side_effects=True, vmem_limit_bytes=52_000_000
        ),
    )(*[
        pltpu.with_memory_space_constraint(x, pltpu.HBM)
        for x in (tokens, logits, slot_grad, phi_param.reshape(4, own // 4, slots))
    ])


def plain(tokens, logits, slot_grad, phi_param):
    inputs = tokens[0]
    scores = logits[0].astype(jnp.float32)
    upstream, phi_full = (
        lax.all_gather(slot_grad[0], "seq", axis=0, tiled=True),
        lax.all_gather(phi_param, "seq", axis=0, tiled=True),
    )
    weight_grad = lax.dot_general(
        inputs, upstream, (((1,), (1,)), ((), ())), preferred_element_type=jnp.float32
    )
    col_peak = lax.pmax(jnp.max(scores, axis=0, keepdims=True), "seq")
    raw_weights = jnp.exp(scores - col_peak)
    col_total = lax.psum(jnp.sum(raw_weights, axis=0, keepdims=True), "seq")
    dispatch = raw_weights / col_total
    col_dot = lax.psum(jnp.sum(dispatch * weight_grad, axis=0, keepdims=True), "seq")
    logit_grad = (dispatch * (weight_grad - col_dot)).astype(jnp.bfloat16)
    dispatch_low = dispatch.astype(jnp.bfloat16)
    grad_scale = float(lax.axis_size("seq") * inputs.shape[0] // 16)
    token_sum = jnp.dot(dispatch_low, upstream, preferred_element_type=jnp.float32)
    token_sum = token_sum + lax.dot_general(
        logit_grad, phi_full, (((1,), (1,)), ((), ())), preferred_element_type=jnp.float32
    )
    token_grad = (grad_scale * token_sum).astype(jnp.bfloat16)[None]
    phi_terms = lax.dot_general(
        inputs, logit_grad, (((0,), (0,)), ((), ())), preferred_element_type=jnp.float32
    )
    phi_share = lax.psum_scatter(phi_terms, "seq", scatter_dimension=0, tiled=True)
    phi_grad = lax.psum(phi_share, "batch")
    return (token_grad, phi_grad)


def per_device(n, batches, tokens, logits, slot_grad, phi_param):
    own, slots = phi_param.shape
    if batches == 4 and n % 8 == 0 and slot_grad.shape[1] % 16 == 0 and own % 128 == 0 and slots % 128 == 0 and tokens.shape[1] % 256 == 0:
        token_grad, phi_grad = fused(n, tokens[0], logits[0], slot_grad[0], phi_param)
        return token_grad[None], phi_grad
    return plain(tokens, logits, slot_grad, phi_param)


def solution(mesh):
    return jax.shard_map(
        functools.partial(per_device, mesh.shape["seq"], mesh.shape["batch"]),
        mesh=mesh,
        in_specs=(
            P("batch", "seq", None),
            P("batch", "seq", None),
            P("batch", "seq", None),
            P("seq", None),
        ),
        out_specs=(P("batch", "seq", None), P("seq", None)),
        check_vma=False,
    )
```
